32 devices in a mesh: gx: 4 (over z), gy: 2 (over x), gz: 4 (over y, core).
Axes of the slice: x: 2, y: 2, z: 4, core: 2. Of those that a mesh axis runs over, the one named last changes fastest.
Arguments:
- amplitudes: float32 [2, 8388608], P(None, ('gx', 'gy', 'gz')), may hold values from -6 to 6
- couplings: float32 [23], replicated, may hold values from -1.2 to 1.2
- fields: float32 [23], replicated, may hold values from 0.3 to 1.2
Outputs:
- evolved: float32 [2, 8388608], P(None, ('gx', 'gy', 'gz'))
The draws below stay inside these ranges and needn't reach their ends.
All inputs are finite; a program needn't handle non-finite values.
Results may differ from the reference program's by a relative error of at most 0.000098.
Values sent between devices are 32-bit elements; how exact they have to be, the bound alone decides.
A program may use at most 64 MiB of HBM per device.

```python
import jax
import jax.numpy as jnp

NQ = 23
NAMP = 8388608


def levels(rng, shape, shards, least, high):
    factor_of, own = 1.0, jax.random.fold_in(rng, 6)
    for axis_at, parts in shards:
        heights = jnp.exp(jax.random.uniform(jax.random.fold_in(own, axis_at), (parts,), jnp.float32, least / len(shards), high / len(shards)))
        factor_of = factor_of * jnp.repeat(heights, shape[axis_at] // parts).reshape([-1 if axis == axis_at else 1 for axis in range(len(shape))])
    return factor_of


def normal_values(own_key, shape, width, most, shards=(), held_as=jnp.bfloat16):
    level = levels(own_key, shape, shards, -0.22, 0.18) if shards else 1.0
    entries = jax.random.normal(own_key, shape, jnp.float32) * width * level
    return jnp.minimum(jnp.maximum(entries, -most), most).astype(held_as)


def setup_inputs(seed: int = 0) -> dict:
    arg_keys = jax.random.split(jax.random.key(seed), 4)
    amplitudes = normal_values(arg_keys[0], (2, NAMP), 1.0, 6.0, ((1, 32),), jnp.float32)
    couplings = jnp.clip(jax.random.uniform(arg_keys[1], (NQ,), jnp.float32, -1.2, 1.2), -1.2, 1.2)
    fields = jnp.clip(jax.random.uniform(arg_keys[2], (NQ,), jnp.float32, 0.3, 1.2), 0.3, 1.2)
    return {"amplitudes": amplitudes, "couplings": couplings, "fields": fields}


def zz_phases(amplitudes, couplings):
    length_all = amplitudes.shape[1]
    qubits = couplings.shape[0]
    positions = jnp.arange(length_all, dtype=jnp.int32)
    phases = jnp.zeros((length_all,), jnp.float32)
    for bond_index in range(qubits):
        follow = (bond_index + 1) % qubits
        parity = ((positions >> bond_index) ^ (positions >> follow)) & 1
        phases = phases + couplings[bond_index] * (1.0 - 2.0 * parity.astype(jnp.float32))
    cos_phase = jnp.cos(phases)
    sin_phase = jnp.sin(phases)
    real_part = amplitudes[0] * cos_phase + amplitudes[1] * sin_phase
    imag_part = amplitudes[1] * cos_phase - amplitudes[0] * sin_phase
    return real_part, imag_part


def rotate_all(real_part, imag_part, fields):
    length_all = real_part.shape[0]
    for qubit_index in range(fields.shape[0]):
        cosine = jnp.cos(fields[qubit_index])
        sine_value = jnp.sin(fields[qubit_index])
        shape_now = (length_all >> (qubit_index + 1), 2, 1 << qubit_index)
        shaped_real = real_part.reshape(shape_now)
        shaped_imag = imag_part.reshape(shape_now)
        lower_real = shaped_real[:, 0]
        upper_real = shaped_real[:, 1]
        lower_imag = shaped_imag[:, 0]
        upper_imag = shaped_imag[:, 1]
        new_lower_real = cosine * lower_real + sine_value * upper_imag
        new_lower_imag = cosine * lower_imag - sine_value * upper_real
        new_upper_real = cosine * upper_real + sine_value * lower_imag
        new_upper_imag = cosine * upper_imag - sine_value * lower_real
        real_part = jnp.stack([new_lower_real, new_upper_real], axis=1).reshape(length_all)
        imag_part = jnp.stack([new_lower_imag, new_upper_imag], axis=1).reshape(length_all)
    return real_part, imag_part


def reference(amplitudes, couplings, fields):
    real_part, imag_part = zz_phases(amplitudes, couplings)
    real_part, imag_part = rotate_all(real_part, imag_part, fields)
    return jnp.stack([real_part, imag_part])
```

```python
import functools
import math

import jax
import jax.numpy as jnp
from jax import lax
from jax.experimental import pallas as pl
from jax.experimental.pallas import tpu as pltpu
from jax.sharding import PartitionSpec as P

MESH = pl.DeviceIdType.MESH
AXES = ("gx", "gy", "gz")
LANES = 128
CHUNK_BITS = 3
TAIL_PARTS = 8
AHEAD = 3
VMEM = 67043328
EXACT = lax.Precision.HIGHEST


def log2(size):
    return size.bit_length() - 1


def bits_set(value, first, last):
    total = jnp.zeros_like(value)
    for bit in range(first, last):
        total = total + ((value >> bit) & 1)
    return total


def swapped(value):
    rows = value.shape[0]
    even = lax.broadcasted_iota(jnp.int32, value.shape, 0) & 1 == 0
    return jnp.where(even, pltpu.roll(value, rows - 1, 0), pltpu.roll(value, 1, 0))


def kernel(sizes, qubits, couplings_at, fields_at, amp, done, held, mid, state, landed, back, low_c, low_s, high_c, high_s, cosine, sine, rows_w, lanes_w, couplings, fields, angle_sem, in_sem, own_sem, out_send, out_recv, near_send, near_recv, back_send, back_recv):
    parts, chunks, sub, _ = held.shape
    part_bits, chunk_bits = log2(parts), log2(chunks)
    lane_bits = log2(LANES)
    inner = lane_bits + log2(sub // 2)
    local_bits = inner + chunk_bits + part_bits
    far_first = qubits - part_bits
    chunk = parts * sub
    place = {axis: lax.axis_index(axis) for axis in AXES}
    me = place["gx"]
    near_at = place["gy"] * sizes["gz"] + place["gz"]

    stages = {axis: [] for axis in AXES}
    qubit = local_bits
    for axis in reversed(AXES):
        for bit in range(log2(sizes[axis])):
            stages[axis].append((axis, bit, qubit))
            qubit += 1
    near = stages["gy"] + list(reversed(stages["gz"]))
    plans = (near, near[1::-1] + near[2:])
    count = len(near)
    others = range(parts - 1)

    def partner(axis, bit):
        return tuple(place[a] ^ (1 << bit) if a == axis else place[a] for a in AXES)

    def other(n):
        return n + jnp.where(me <= n, 1, 0)

    def across(target):
        return tuple(target if a == "gx" else place[a] for a in AXES)

    def settle(ref, sem):
        pltpu.make_async_copy(ref, ref, sem).wait()

    loads = [pltpu.make_async_copy(amp.at[:, c], held.at[:, c], in_sem.at[min(c, 1)]) for c in range(chunks)]
    owns = [pltpu.make_async_copy(amp.at[me, c], mid.at[c, me], own_sem) for c in range(chunks)]
    barrier = pltpu.get_barrier_semaphore()
    for n in others:
        pl.semaphore_signal(barrier, inc=1, device_id=across(other(n)), device_id_type=MESH)
    for axis, bit, _ in near:
        pl.semaphore_signal(barrier, inc=1, device_id=partner(axis, bit), device_id_type=MESH)
    for load in loads:
        load.start()
    for own in owns:
        own.start()
    angles = [pltpu.make_async_copy(couplings_at, couplings, angle_sem.at[0]), pltpu.make_async_copy(fields_at, fields, angle_sem.at[1])]
    for angle in angles:
        angle.start()

    def out(c, n):
        target = other(n)
        return pltpu.make_async_remote_copy(
            src_ref=held.at[target, c],
            dst_ref=mid.at[c, me],
            send_sem=out_send,
            recv_sem=out_recv.at[c],
            device_id=across(target),
            device_id_type=MESH,
        )

    def send(c, k):
        axis, bit, _ = plans[c % 2][k]
        return pltpu.make_async_remote_copy(
            src_ref=state.at[k, c],
            dst_ref=landed.at[k, c],
            send_sem=near_send,
            recv_sem=near_recv.at[k, c],
            device_id=partner(axis, bit),
            device_id_type=MESH,
        )

    tail = sub // TAIL_PARTS
    late = chunks - 2
    groups = [(c, 1, 0, sub) for c in range(late)] + [(late, 2, t * tail, tail) for t in range(TAIL_PARTS)]
    arrivals = [0] * (late // 2) + [1] * (late - late // 2) + [2 + t for t in range(TAIL_PARTS)]

    def give(g, n):
        c, size, first, length = groups[g]
        span = pl.ds(first, length)
        target = other(n)
        return pltpu.make_async_remote_copy(
            src_ref=state.at[count, pl.ds(c, size), target, span],
            dst_ref=back.at[me, pl.ds(c, size), span],
            send_sem=back_send,
            recv_sem=back_recv.at[arrivals[g]],
            device_id=across(target),
            device_id_type=MESH,
        )

    pl.semaphore_wait(barrier, len(others) + count)
    for c in range(AHEAD):
        if c == 0:
            loads[c].wait()
        elif c == 1:
            settle(held.at[:, pl.ds(1, chunks - 1)], in_sem.at[1])
        for n in others:
            out(c, n).start()
    for angle in angles:
        angle.wait()

    for q in range(qubits):
        cosine[pl.ds(q, 1), :] = jnp.full((1, LANES), fields[q], jnp.float32)
    angles = cosine[...]
    cosine[...] = jnp.cos(angles)
    sine[...] = jnp.sin(angles)

    def angle_of(position, bonds):
        total = jnp.zeros(position.shape, jnp.float32)
        for q in bonds:
            parity = (position >> q ^ position >> ((q + 1) % qubits)) & 1
            total = total + couplings[q] * (1.0 - 2.0 * parity.astype(jnp.float32))
        return total

    quarter = math.pi / 2
    row = lax.broadcasted_iota(jnp.int32, (2 * sub, LANES), 0)
    lane = lax.broadcasted_iota(jnp.int32, (2 * sub, LANES), 1)
    top = jnp.where(row >= sub, 1, 0)
    position = (top << (qubits - 1)) + (((row - top * sub) >> 1) << lane_bits) + lane
    turns = bits_set(position, 0, inner) & 3
    low = angle_of(position, list(range(inner - 1)) + [qubits - 1]) + turns.astype(jnp.float32) * quarter
    low_c[...] = jnp.cos(low)
    low_s[...] = jnp.sin(low)
    number = lax.broadcasted_iota(jnp.int32, (2 * parts * chunks, LANES), 0)
    position = (
        ((number >> (1 + chunk_bits)) << far_first)
        + (near_at << local_bits)
        + (me << (inner + chunk_bits))
        + (((number >> 1) & (chunks - 1)) << inner)
        + ((number & 1) << (inner - 1))
    )
    turns = bits_set(position, inner, qubits) & 3
    high = angle_of(position, range(inner - 1, qubits - 1)) + turns.astype(jnp.float32) * quarter
    high_c[...] = jnp.cos(high)
    high_s[...] = jnp.sin(high)

    def matrix(shape, first_row, skip, mixed):
        there = lax.broadcasted_iota(jnp.int32, shape, 0) + first_row
        here = lax.broadcasted_iota(jnp.int32, shape, 1)
        total = jnp.ones(shape, jnp.float32)
        if skip:
            total = jnp.where((there ^ here) & ((1 << skip) - 1) == 0, total, 0.0)
        repeat = shape[1] // LANES
        for at, q in enumerate(mixed):
            bit = at + skip
            c_q = jnp.concatenate([cosine[pl.ds(q, 1), :]] * repeat, axis=1)
            s_q = jnp.concatenate([sine[pl.ds(q, 1), :]] * repeat, axis=1)
            up, left = there >> bit & 1, here >> bit & 1
            total = total * jnp.where(up ^ left == 1, s_q, jnp.where(up == 1, -c_q, c_q))
        return total

    lanes_w[...] = matrix((LANES, LANES), 0, 0, range(lane_bits))

    @pl.loop(0, chunk // 8)
    def _(step):
        at = pl.multiple_of(step * 8, 8)
        rows_w[pl.ds(at, 8), :] = matrix((8, chunk), at, 1, list(range(lane_bits, inner)) + list(range(far_first, qubits)))

    def turn(c):
        @pl.loop(0, sub // 8)
        def _(step):
            sign = jnp.where(lax.broadcasted_iota(jnp.int32, (8, LANES), 0) & 1 == 0, 1.0, -1.0)
            at = pl.multiple_of(step * 8, 8)
            half = step * 16 // sub
            for p in range(parts):
                c_low = low_c[pl.ds(pl.multiple_of(p * 2 // parts * sub + at, 8), 8), :]
                s_low = low_s[pl.ds(pl.multiple_of(p * 2 // parts * sub + at, 8), 8), :]
                which = (p * chunks + c) * 2 + half
                c_high = high_c[pl.ds(which, 1), :]
                s_high = high_s[pl.ds(which, 1), :]
                value = mid[c, p, pl.ds(at, 8), :]
                c_all = c_low * c_high - s_low * s_high
                s_all = s_low * c_high + c_low * s_high
                mid[c, p, pl.ds(at, 8), :] = value * c_all + swapped(value) * (s_all * sign)

    def local(c):
        for p in range(parts):
            mid[c, p] = jnp.dot(mid[c, p], lanes_w[...], precision=EXACT, preferred_element_type=jnp.float32)

        @pl.loop(0, parts)
        def _(p):
            at = pl.multiple_of(p * sub, sub)
            state[0, c, p] = jnp.dot(
                rows_w[pl.ds(at, sub), :], mid[c].reshape(chunk, LANES), precision=EXACT, preferred_element_type=jnp.float32
            )

    def combine(c, k):
        axis, bit, q = plans[c % 2][k]
        own = 1.0 - 2.0 * ((place[axis] >> bit) & 1).astype(jnp.float32)

        @pl.loop(0, sub // 16)
        def _(step):
            at = pl.multiple_of(step * 16, 16)
            c_q = cosine[pl.ds(q, 1), :] * own
            s_q = sine[pl.ds(q, 1), :]
            if k == count - 1:
                row = lax.broadcasted_iota(jnp.int32, (16, LANES), 0) + at
                lane = lax.broadcasted_iota(jnp.int32, (16, LANES), 1)
                inside = bits_set(((row >> 1) << lane_bits) + lane, 0, inner) + bits_set(near_at, 0, far_first - local_bits)
            for p in range(parts):
                value = c_q * state[k, c, p, pl.ds(at, 16), :] + s_q * landed[k, c, p, pl.ds(at, 16), :]
                if k == count - 1:
                    turns = inside + p.bit_count()
                    value = jnp.where(turns & 1 == 1, swapped(value), value)
                    value = jnp.where((turns + (row & 1)) & 2 == 2, -value, value)
                state[k + 1, c, p, pl.ds(at, 16), :] = value

    def keep(c):
        back[me, c] = state[count, c, me]

    events = [(c + (2 * k if k < count else 2 * k - 1.5), k, c) for c in range(chunks) for k in range(count + 1)]
    for _, k, c in sorted(events):
        if k == 0:
            if c == 0:
                settle(mid.at[:, 0], own_sem)
            settle(mid.at[c, pl.ds(0, parts - 1)], out_recv.at[c])
            if c + AHEAD < chunks:
                for n in others:
                    out(c + AHEAD, n).start()
            turn(c)
            local(c)
            send(c, 0).start()
        else:
            send(c, k - 1).wait_recv()
            combine(c, k - 1)
            if k < count:
                send(c, k).start()
            else:
                for n in others:
                    for g, group in enumerate(groups):
                        if group[0] + group[1] - 1 == c:
                            give(g, n).start()
                keep(c)

    settle(held.at[pl.ds(0, parts - 1)], out_send)
    settle(state.at[pl.ds(0, count)], near_send)

    def fold(values, bits, where):
        for bit in bits:
            c_q = cosine[pl.ds(inner + bit, 1), :]
            s_q = sine[pl.ds(inner + bit, 1), :]
            for n in where:
                if not n >> bit & 1:
                    one, two = values[n], values[n | 1 << bit]
                    values[n] = c_q * one + s_q * two
                    values[n | 1 << bit] = s_q * one - c_q * two

    part_span = range(chunk_bits, chunk_bits + part_bits)

    def early(first, length):
        where = [p * chunks + c for p in range(parts) for c in range(first, first + length)]
        inside = [bit for bit in range(chunk_bits) if length >> (bit + 1) and first % (2 << bit) == 0]

        @pl.loop(0, sub // 8)
        def _(step):
            at = pl.multiple_of(step * 8, 8)
            values = {n: back[n // chunks, n % chunks, pl.ds(at, 8), :] for n in where}
            fold(values, inside, where)
            fold(values, part_span, where)
            for n in where:
                back[n // chunks, n % chunks, pl.ds(at, 8), :] = values[n]

    def finish(first, size):
        @pl.loop(0, size // 8)
        def _(step):
            at = pl.multiple_of(first + step * 8, 8)
            sign = jnp.where(lax.broadcasted_iota(jnp.int32, (8, LANES), 0) & 1 == 0, 1.0, -1.0)
            values = [back[n // chunks, n % chunks, pl.ds(at, 8), :] for n in range(parts * chunks)]
            last = [n for n in range(parts * chunks) if n % chunks >= late]
            fold(values, part_span, last)
            fold(values, [0], last)
            for bit in range(1, chunk_bits):
                fold(values, [bit], [n for n in range(parts * chunks) if n % chunks >= chunks - (2 << bit)])
            for n, value in enumerate(values):
                turns = n.bit_count() & 3
                if turns & 1:
                    value = swapped(value) * (sign if turns == 1 else -sign)
                elif turns == 2:
                    value = -value
                done[n // chunks, n % chunks, pl.ds(at, 8), :] = value

    start = 0
    size = chunks // 2
    while start < late:
        if start == 0:
            settle(back.at[pl.ds(0, parts - 1), pl.ds(0, late // 2)], back_recv.at[0])
            settle(back.at[pl.ds(0, parts - 1), pl.ds(late // 2, late - late // 2)], back_recv.at[1])
        early(start, size)
        start += size
        size //= 2
    for t in range(TAIL_PARTS):
        settle(back.at[pl.ds(0, parts - 1), pl.ds(late, 2), pl.ds(t * tail, tail)], back_recv.at[2 + t])
        finish(t * tail, tail)
    settle(back.at[pl.ds(0, parts - 1)], back_send)


def solution(mesh):
    sizes = {axis: mesh.shape[axis] for axis in AXES}
    count = sum(log2(sizes[axis]) for axis in AXES[1:])

    def step(amplitudes, couplings, fields):
        local = amplitudes.shape[1]
        qubits = couplings.shape[0]
        rows = 2 * local // LANES
        parts = sizes[AXES[0]]
        chunks = 1 << CHUNK_BITS
        sub = rows // (parts * chunks)
        chunk = parts * sub
        table = -(-qubits // 8) * 8
        shape = (parts, chunks, sub, LANES)
        turned = (chunks, parts, sub, LANES)
        woven = amplitudes.reshape(2, local // LANES, LANES).transpose(1, 0, 2).reshape(shape)
        vmem = lambda *shape: pltpu.VMEM(shape, jnp.float32)
        dma = lambda *shape: pltpu.SemaphoreType.DMA(shape)
        result = pl.pallas_call(
            functools.partial(kernel, sizes, qubits),
            out_shape=pltpu.VMEM(shape, jnp.float32),
            in_specs=[pl.BlockSpec(memory_space=pltpu.HBM)] * 3,
            out_specs=pl.BlockSpec(memory_space=pltpu.VMEM),
            scratch_shapes=[
                vmem(*shape),
                vmem(*turned),
                vmem(count + 1, *turned),
                vmem(count, *turned),
                vmem(*shape),
                vmem(2 * sub, LANES),
                vmem(2 * sub, LANES),
                vmem(2 * parts * chunks, LANES),
                vmem(2 * parts * chunks, LANES),
                vmem(table, LANES),
                vmem(table, LANES),
                vmem(chunk, chunk),
                vmem(LANES, LANES),
                pltpu.SMEM((qubits,), jnp.float32),
                pltpu.SMEM((qubits,), jnp.float32),
                dma(2),
                dma(2),
                pltpu.SemaphoreType.DMA,
                pltpu.SemaphoreType.DMA,
                dma(chunks),
                pltpu.SemaphoreType.DMA,
                dma(count, chunks),
                pltpu.SemaphoreType.DMA,
                dma(2 + TAIL_PARTS),
            ],
            compiler_params=pltpu.CompilerParams(
                collective_id=0, has_side_effects=True, vmem_limit_bytes=VMEM - 4 * rows * LANES
            ),
        )(couplings, fields, woven)
        return result.reshape(local // LANES, 2, LANES).transpose(1, 0, 2).reshape(2, local)

    placed = (P(None, AXES), P(), P())
    return jax.shard_map(step, mesh=mesh, in_specs=placed, out_specs=P(None, AXES), check_vma=False)
```

```python
import functools
import math

import jax
import jax.numpy as jnp
from jax import lax
from jax.experimental import pallas as pl
from jax.experimental.pallas import tpu as pltpu
from jax.sharding import PartitionSpec as P

MESH = pl.DeviceIdType.MESH
AXES = ("gx", "gy", "gz")
LANES = 128
CHUNK_BITS = 3
TAIL_PARTS = 8
AHEAD = 4
STEP = 1.6
VMEM = 67043328
EXACT = lax.Precision.HIGHEST


def log2(size):
    return size.bit_length() - 1


def bits_set(value, first, last):
    total = jnp.zeros_like(value)
    for bit in range(first, last):
        total = total + ((value >> bit) & 1)
    return total


def swapped(value):
    rows = value.shape[0]
    even = lax.broadcasted_iota(jnp.int32, value.shape, 0) & 1 == 0
    return jnp.where(even, pltpu.roll(value, rows - 1, 0), pltpu.roll(value, 1, 0))


def kernel(sizes, qubits, couplings_at, fields_at, amp, done, held, mid, state, landed, final, back, low_c, low_s, high_c, high_s, cosine, sine, rows_w, lanes_w, couplings, fields, far_ready, near_ready, angle_sem, in_sem, own_sem, out_send, out_recv, near_send, near_recv, back_send, back_recv):
    parts, chunks, sub, _ = held.shape
    part_bits, chunk_bits = log2(parts), log2(chunks)
    lane_bits = log2(LANES)
    inner = lane_bits + log2(sub // 2)
    local_bits = inner + chunk_bits + part_bits
    far_first = qubits - part_bits
    chunk = parts * sub
    place = {axis: lax.axis_index(axis) for axis in AXES}
    me = place["gx"]
    near_at = place["gy"] * sizes["gz"] + place["gz"]

    stages = {axis: [] for axis in AXES}
    qubit = local_bits
    for axis in reversed(AXES):
        for bit in range(log2(sizes[axis])):
            stages[axis].append((axis, bit, qubit))
            qubit += 1
    near = stages["gy"] + list(reversed(stages["gz"]))
    plans = (near, near[1::-1] + near[2:])
    count = len(near)
    others = range(parts - 1)
    late = chunks - 2

    def partner(axis, bit):
        return tuple(place[a] ^ (1 << bit) if a == axis else place[a] for a in AXES)

    def other(n, mirrored=True):
        mirror = me < parts // 2
        seen = jnp.where(mirror, parts - 1 - me, me) if mirrored else me
        target = n + jnp.where(seen <= n, 1, 0)
        return jnp.where(mirror, parts - 1 - target, target) if mirrored else target

    def across(target):
        return tuple(target if a == "gx" else place[a] for a in AXES)

    def settle(ref, sem):
        pltpu.make_async_copy(ref, ref, sem).wait()

    loads = [pltpu.make_async_copy(amp.at[:, c], held.at[:, c], in_sem.at[min(c, 1)]) for c in range(chunks)]
    owns = [pltpu.make_async_copy(amp.at[me, c], mid.at[c, me], own_sem) for c in range(late)]
    barrier = pltpu.get_barrier_semaphore()
    for n in others:
        target = other(n)

        @pl.when(jnp.logical_or(target > me, target < parts // 2))
        def _():
            pl.semaphore_signal(barrier, inc=1, device_id=across(target), device_id_type=MESH)

    below = [place[axis] >> bit & 1 for axis, bit, _ in near]
    for down, (axis, bit, _) in zip(below, near):

        @pl.when(down == 0)
        def _():
            pl.semaphore_signal(barrier, inc=1, device_id=partner(axis, bit), device_id_type=MESH)

    for load in loads:
        load.start()
    for own in owns:
        own.start()
    angles = [pltpu.make_async_copy(couplings_at, couplings, angle_sem.at[0]), pltpu.make_async_copy(fields_at, fields, angle_sem.at[1])]
    for angle in angles:
        angle.start()
    pl.semaphore_wait(barrier, sum(below) + jnp.where(me < parts // 2, parts - 1, me))
    for n in others:
        target = other(n)

        @pl.when(jnp.logical_and(target < me, target >= parts // 2))
        def _():
            pl.semaphore_signal(far_ready.at[me], inc=1, device_id=across(target), device_id_type=MESH)

    def out(c, n):
        target = other(n)
        return pltpu.make_async_remote_copy(
            src_ref=held.at[target, c] if c < late else state.at[count, c, target],
            dst_ref=mid.at[c, me],
            send_sem=out_send,
            recv_sem=out_recv.at[c],
            device_id=across(target),
            device_id_type=MESH,
        )

    def send(c, k):
        axis, bit, _ = plans[c % 2][k]
        return pltpu.make_async_remote_copy(
            src_ref=state.at[k, c],
            dst_ref=landed.at[k, c],
            send_sem=near_send,
            recv_sem=near_recv.at[k, c // 2],
            device_id=partner(axis, bit),
            device_id_type=MESH,
        )

    tail = sub // TAIL_PARTS
    groups = [(c, 1, 0, sub) for c in range(late)] + [(late, 2, t * tail, tail) for t in range(TAIL_PARTS)]
    pairs = late // 2
    arrivals = [c // 2 for c in range(late)] + [pairs + t for t in range(TAIL_PARTS)]

    def give(g, n):
        c, size, first, length = groups[g]
        span = pl.ds(first, length)
        target = other(n, c < late)
        return pltpu.make_async_remote_copy(
            src_ref=state.at[count, pl.ds(c, size), target, span] if c < late else final.at[:, target, span],
            dst_ref=back.at[me, pl.ds(c, size), span],
            send_sem=back_send,
            recv_sem=back_recv.at[arrivals[g]],
            device_id=across(target),
            device_id_type=MESH,
        )

    def first(low):
        for c in range(AHEAD):
            if low and c == 0:
                loads[c].wait()
            elif low and c == 1:
                settle(held.at[:, pl.ds(1, chunks - 1)], in_sem.at[1])
            for n in others:
                target = other(n)

                known = jnp.logical_or(target < me, me < parts // 2)

                @pl.when(known if low else jnp.logical_not(known))
                def _():
                    if not low and c == 0:
                        pl.semaphore_wait(far_ready.at[target], 1)
                    out(c, n).start()

    first(True)
    for down, (axis, bit, _) in zip(below, near):

        @pl.when(down == 1)
        def _():
            pl.semaphore_signal(near_ready, inc=1, device_id=partner(axis, bit), device_id_type=MESH)

    for angle in angles:
        angle.wait()

    for q in range(qubits):
        cosine[pl.ds(q, 1), :] = jnp.full((1, LANES), fields[q], jnp.float32)
    angles = cosine[...]
    cosine[...] = jnp.cos(angles)
    sine[...] = jnp.sin(angles)

    def angle_of(position, bonds):
        total = jnp.zeros(position.shape, jnp.float32)
        for q in bonds:
            parity = (position >> q ^ position >> ((q + 1) % qubits)) & 1
            total = total + couplings[q] * (1.0 - 2.0 * parity.astype(jnp.float32))
        return total

    quarter = math.pi / 2
    row = lax.broadcasted_iota(jnp.int32, (2 * sub, LANES), 0)
    lane = lax.broadcasted_iota(jnp.int32, (2 * sub, LANES), 1)
    top = jnp.where(row >= sub, 1, 0)
    position = (top << (qubits - 1)) + (((row - top * sub) >> 1) << lane_bits) + lane
    turns = bits_set(position, 0, inner) & 3
    low = angle_of(position, list(range(inner - 1)) + [qubits - 1]) + turns.astype(jnp.float32) * quarter
    low_c[...] = jnp.cos(low)
    low_s[...] = jnp.sin(low)
    table = 2 * parts * chunks
    number = lax.broadcasted_iota(jnp.int32, high_c.shape, 0)
    rest = number - table
    before = rest >= 0
    position = (
        (jnp.where(before, me, number >> (1 + chunk_bits)) << far_first)
        + (near_at << local_bits)
        + (jnp.where(before, rest >> 2, me) << (inner + chunk_bits))
        + (jnp.where(before, late + (rest >> 1 & 1), (number >> 1) & (chunks - 1)) << inner)
        + ((number & 1) << (inner - 1))
    )
    turns = bits_set(position, inner, qubits) & 3
    high = angle_of(position, range(inner - 1, qubits - 1)) + turns.astype(jnp.float32) * quarter
    high_c[...] = jnp.cos(high)
    high_s[...] = jnp.sin(high)
    first(False)

    def turned(value, low_at, high_at):
        sign = jnp.where(lax.broadcasted_iota(jnp.int32, (8, LANES), 0) & 1 == 0, 1.0, -1.0)
        c_low = low_c[pl.ds(pl.multiple_of(low_at, 8), 8), :]
        s_low = low_s[pl.ds(pl.multiple_of(low_at, 8), 8), :]
        c_high = high_c[pl.ds(high_at, 1), :]
        s_high = high_s[pl.ds(high_at, 1), :]
        c_all = c_low * c_high - s_low * s_high
        s_all = s_low * c_high + c_low * s_high
        return value * c_all + swapped(value) * (s_all * sign)

    @pl.loop(0, sub // 8)
    def _(step):
        at = pl.multiple_of(step * 8, 8)
        half = step * 16 // sub
        for c in (late, late + 1):
            for p in range(parts):
                high_at = table + p * 4 + (c - late) * 2 + half
                state[0, c, p, pl.ds(at, 8), :] = turned(held[p, c, pl.ds(at, 8), :], me * 2 // parts * sub + at, high_at)

    @pl.when(sum(below) < count)
    def _():
        pl.semaphore_wait(near_ready, count - sum(below))

    for c in (late, late + 1):
        send(c, 0).start()

    def matrix(shape, first_row, skip, mixed):
        there = lax.broadcasted_iota(jnp.int32, shape, 0) + first_row
        here = lax.broadcasted_iota(jnp.int32, shape, 1)
        total = jnp.ones(shape, jnp.float32)
        if skip:
            total = jnp.where((there ^ here) & ((1 << skip) - 1) == 0, total, 0.0)
        repeat = shape[1] // LANES
        for at, q in enumerate(mixed):
            bit = at + skip
            c_q = jnp.concatenate([cosine[pl.ds(q, 1), :]] * repeat, axis=1)
            s_q = jnp.concatenate([sine[pl.ds(q, 1), :]] * repeat, axis=1)
            up, left = there >> bit & 1, here >> bit & 1
            total = total * jnp.where(up ^ left == 1, s_q, jnp.where(up == 1, -c_q, c_q))
        return total

    lanes_w[...] = matrix((LANES, LANES), 0, 0, range(lane_bits))

    @pl.loop(0, chunk // 8)
    def _(step):
        at = pl.multiple_of(step * 8, 8)
        rows_w[pl.ds(at, 8), :] = matrix((8, chunk), at, 1, list(range(lane_bits, inner)) + list(range(far_first, qubits)))

    def turn(c):
        @pl.loop(0, sub // 8)
        def _(step):
            at = pl.multiple_of(step * 8, 8)
            half = step * 16 // sub
            for p in range(parts):
                mid[c, p, pl.ds(at, 8), :] = turned(mid[c, p, pl.ds(at, 8), :], p * 2 // parts * sub + at, (p * chunks + c) * 2 + half)

    def local(c, target):
        for p in range(parts):
            mid[c, p] = jnp.dot(mid[c, p], lanes_w[...], precision=EXACT, preferred_element_type=jnp.float32)

        @pl.loop(0, parts)
        def _(p):
            at = pl.multiple_of(p * sub, sub)
            target[p] = jnp.dot(
                rows_w[pl.ds(at, sub), :], mid[c].reshape(chunk, LANES), precision=EXACT, preferred_element_type=jnp.float32
            )

    def each_part(step, source, target, straight):
        at = pl.multiple_of(step * 16, 16)
        row = lax.broadcasted_iota(jnp.int32, (16, LANES), 0) + at
        lane = lax.broadcasted_iota(jnp.int32, (16, LANES), 1)
        inside = bits_set(((row >> 1) << lane_bits) + lane, 0, inner) + bits_set(near_at, 0, far_first - local_bits)
        for p in range(parts):
            value = source(p, at)
            if straight:
                turns = inside + p.bit_count()
                value = jnp.where(turns & 1 == 1, swapped(value), value)
                value = jnp.where((turns + (row & 1)) & 2 == 2, -value, value)
            target[p, pl.ds(at, 16), :] = value

    def combine(c, k):
        axis, bit, q = plans[c % 2][k]
        own = 1.0 - 2.0 * ((place[axis] >> bit) & 1).astype(jnp.float32)

        @pl.loop(0, sub // 16)
        def _(step):
            c_q = cosine[pl.ds(q, 1), :] * own
            s_q = sine[pl.ds(q, 1), :]
            source = lambda p, at: c_q * state[k, c, p, pl.ds(at, 16), :] + s_q * landed[k, c, p, pl.ds(at, 16), :]
            each_part(step, source, state.at[k + 1, c], k == count - 1 and c < late)

    def straighten(ref):
        @pl.loop(0, sub // 16)
        def _(step):
            each_part(step, lambda p, at: ref[p, pl.ds(at, 16), :], ref, True)

    def return_all(c):
        sends = [(g, n) for n in others for g, group in enumerate(groups) if group[0] + group[1] - 1 == c]
        for g, n in sends:
            give(g, n).start()

    ARRIVE, MEET, LEAVE = range(3)
    events = [(c, ARRIVE, c, 0) for c in range(chunks)]
    for c in range(1, late, 2):
        events += [(c + STEP * min(k, count - 1) + k // count * 0.2, MEET, c, k) for k in range(1, count + 1)]
    events += [(min(k, count - 1) - 1.5 + k // count * 0.1, MEET, chunks - 1, k) for k in range(1, count + 1)]
    events.append((4 * chunks, LEAVE, chunks - 1, 0))
    for _, what, c, k in sorted(events):
        if what == ARRIVE:
            if c == 0:
                settle(mid.at[pl.ds(0, late), 0], own_sem)
            settle(mid.at[c, pl.ds(0, parts - 1)], out_recv.at[c])
            if c + AHEAD < chunks:
                for n in others:
                    out(c + AHEAD, n).start()
            if c < late:
                turn(c)
                local(c, state.at[0, c])
                send(c, 0).start()
            else:
                mid[c, me] = state[count, c, me]
                local(c, final.at[c - late])
                straighten(final.at[c - late])
                back[me, c] = final[c - late, me]
        elif what == MEET:
            settle(landed.at[k - 1, pl.ds(c - 1, 2)], near_recv.at[k - 1, c // 2])
            for each in (c - 1, c):
                combine(each, k - 1)
                if k < count:
                    send(each, k).start()
                elif c < late:
                    back[me, each] = state[count, each, me]
                    return_all(each)
        else:
            return_all(c)

    settle(mid.at[:, pl.ds(0, parts - 1)], out_send)
    settle(state.at[pl.ds(0, count)], near_send)

    def fold(values, bits, where):
        for bit in bits:
            c_q = cosine[pl.ds(inner + bit, 1), :]
            s_q = sine[pl.ds(inner + bit, 1), :]
            for n in where:
                if not n >> bit & 1:
                    one, two = values[n], values[n | 1 << bit]
                    values[n] = c_q * one + s_q * two
                    values[n | 1 << bit] = s_q * one - c_q * two

    part_span = range(chunk_bits, chunk_bits + part_bits)

    def early(first, length):
        where = [p * chunks + c for p in range(parts) for c in range(first, first + length)]
        inside = [bit for bit in range(chunk_bits) if length >> (bit + 1) and first % (2 << bit) == 0]

        @pl.loop(0, sub // 8)
        def _(step):
            at = pl.multiple_of(step * 8, 8)
            values = {n: back[n // chunks, n % chunks, pl.ds(at, 8), :] for n in where}
            fold(values, inside, where)
            fold(values, part_span, where)
            for n in where:
                back[n // chunks, n % chunks, pl.ds(at, 8), :] = values[n]

    def finish(first, size):
        @pl.loop(0, size // 8)
        def _(step):
            at = pl.multiple_of(first + step * 8, 8)
            sign = jnp.where(lax.broadcasted_iota(jnp.int32, (8, LANES), 0) & 1 == 0, 1.0, -1.0)
            values = [back[n // chunks, n % chunks, pl.ds(at, 8), :] for n in range(parts * chunks)]
            last = [n for n in range(parts * chunks) if n % chunks >= late]
            fold(values, part_span, last)
            fold(values, [0], last)
            for bit in range(1, chunk_bits):
                fold(values, [bit], [n for n in range(parts * chunks) if n % chunks >= chunks - (2 << bit)])
            for n, value in enumerate(values):
                turns = n.bit_count() & 3
                if turns & 1:
                    value = swapped(value) * (sign if turns == 1 else -sign)
                elif turns == 2:
                    value = -value
                done[n // chunks, n % chunks, pl.ds(at, 8), :] = value

    start, size = 0, chunks // 2
    for pair in range(pairs):
        settle(back.at[pl.ds(0, parts - 1), pl.ds(2 * pair, 2)], back_recv.at[pair])
        if start + size == 2 * pair + 2:
            early(start, size)
            start, size = start + size, size // 2
    for t in range(TAIL_PARTS):
        settle(back.at[pl.ds(0, parts - 1), pl.ds(late, 2), pl.ds(t * tail, tail)], back_recv.at[pairs + t])
        finish(t * tail, tail)
    settle(back.at[pl.ds(0, parts - 1)], back_send)


def solution(mesh):
    sizes = {axis: mesh.shape[axis] for axis in AXES}
    count = sum(log2(sizes[axis]) for axis in AXES[1:])

    def step(amplitudes, couplings, fields):
        local = amplitudes.shape[1]
        qubits = couplings.shape[0]
        rows = 2 * local // LANES
        parts = sizes[AXES[0]]
        chunks = 1 << CHUNK_BITS
        sub = rows // (parts * chunks)
        chunk = parts * sub
        table = -(-qubits // 8) * 8
        shape = (parts, chunks, sub, LANES)
        turned = (chunks, parts, sub, LANES)
        woven = amplitudes.reshape(2, local // LANES, LANES).transpose(1, 0, 2).reshape(shape)
        vmem = lambda *shape: pltpu.VMEM(shape, jnp.float32)
        dma = lambda *shape: pltpu.SemaphoreType.DMA(shape)
        result = pl.pallas_call(
            functools.partial(kernel, sizes, qubits),
            out_shape=pltpu.VMEM(shape, jnp.float32),
            in_specs=[pl.BlockSpec(memory_space=pltpu.HBM)] * 3,
            out_specs=pl.BlockSpec(memory_space=pltpu.VMEM),
            scratch_shapes=[
                vmem(*shape),
                vmem(*turned),
                vmem(count + 1, *turned),
                vmem(count, *turned),
                vmem(2, *turned[1:]),
                vmem(*shape),
                vmem(2 * sub, LANES),
                vmem(2 * sub, LANES),
                vmem(2 * parts * (chunks + 2), LANES),
                vmem(2 * parts * (chunks + 2), LANES),
                vmem(table, LANES),
                vmem(table, LANES),
                vmem(chunk, chunk),
                vmem(LANES, LANES),
                pltpu.SMEM((qubits,), jnp.float32),
                pltpu.SMEM((qubits,), jnp.float32),
                pltpu.SemaphoreType.REGULAR((parts,)),
                pltpu.SemaphoreType.REGULAR,
                dma(2),
                dma(2),
                pltpu.SemaphoreType.DMA,
                pltpu.SemaphoreType.DMA,
                dma(chunks),
                pltpu.SemaphoreType.DMA,
                dma(count, chunks // 2),
                pltpu.SemaphoreType.DMA,
                dma(chunks // 2 - 1 + TAIL_PARTS),
            ],
            compiler_params=pltpu.CompilerParams(
                collective_id=0, has_side_effects=True, vmem_limit_bytes=VMEM - 4 * rows * LANES
            ),
        )(couplings, fields, woven)
        return result.reshape(local // LANES, 2, LANES).transpose(1, 0, 2).reshape(2, local)

    placed = (P(None, AXES), P(), P())
    return jax.shard_map(step, mesh=mesh, in_specs=placed, out_specs=P(None, AXES), check_vma=False)
```

```python
import functools
import math

import jax
import jax.numpy as jnp
from jax import lax
from jax.experimental import pallas as pl
from jax.experimental.pallas import tpu as pltpu
from jax.sharding import PartitionSpec as P

MESH = pl.DeviceIdType.MESH
AXES = ("gx", "gy", "gz")
LANES = 128
CHUNK_BITS = 3
TAIL_PARTS = 8
AHEAD = 4
STEP = 1.6
VMEM = 67043328
EXACT = lax.Precision.HIGHEST


def log2(size):
    return size.bit_length() - 1


def bits_set(value, first, last):
    total = jnp.zeros_like(value)
    for bit in range(first, last):
        total = total + ((value >> bit) & 1)
    return total


def swapped(value):
    rows = value.shape[0]
    even = lax.broadcasted_iota(jnp.int32, value.shape, 0) & 1 == 0
    return jnp.where(even, pltpu.roll(value, rows - 1, 0), pltpu.roll(value, 1, 0))


def kernel(sizes, qubits, couplings_at, fields_at, amp, done, held, mid, state, landed, final, back, low_c, low_s, high_c, high_s, cosine, sine, rows_w, lanes_w, couplings, fields, far_ready, near_ready, angle_sem, in_sem, own_sem, out_send, out_recv, near_send, near_recv, back_send, back_recv):
    parts, chunks, sub, _ = held.shape
    part_bits, chunk_bits = log2(parts), log2(chunks)
    lane_bits = log2(LANES)
    inner = lane_bits + log2(sub // 2)
    local_bits = inner + chunk_bits + part_bits
    far_first = qubits - part_bits
    chunk = parts * sub
    place = {axis: lax.axis_index(axis) for axis in AXES}
    me = place["gx"]
    near_at = place["gy"] * sizes["gz"] + place["gz"]

    stages = {axis: [] for axis in AXES}
    qubit = local_bits
    for axis in reversed(AXES):
        for bit in range(log2(sizes[axis])):
            stages[axis].append((axis, bit, qubit))
            qubit += 1
    near = stages["gy"] + list(reversed(stages["gz"]))
    plans = (near, near[1::-1] + near[2:])
    count = len(near)
    others = range(parts - 1)
    late = chunks - 2

    def partner(axis, bit):
        return tuple(place[a] ^ (1 << bit) if a == axis else place[a] for a in AXES)

    def other(n, mirrored=True):
        mirror = me < parts // 2
        seen = jnp.where(mirror, parts - 1 - me, me) if mirrored else me
        target = n + jnp.where(seen <= n, 1, 0)
        return jnp.where(mirror, parts - 1 - target, target) if mirrored else target

    def across(target):
        return tuple(target if a == "gx" else place[a] for a in AXES)

    def settle(ref, sem):
        pltpu.make_async_copy(ref, ref, sem).wait()

    loads = [pltpu.make_async_copy(amp.at[:, c], held.at[:, c], in_sem.at[min(c, 1)]) for c in range(chunks)]
    owns = [pltpu.make_async_copy(amp.at[me, c], mid.at[c, me], own_sem) for c in range(late)]
    barrier = pltpu.get_barrier_semaphore()
    for n in others:
        target = other(n)

        @pl.when(jnp.logical_or(target > me, target < parts // 2))
        def _():
            pl.semaphore_signal(barrier, inc=1, device_id=across(target), device_id_type=MESH)

    below = [place[axis] >> bit & 1 for axis, bit, _ in near]
    for down, (axis, bit, _) in zip(below, near):

        @pl.when(down == 0)
        def _():
            pl.semaphore_signal(barrier, inc=1, device_id=partner(axis, bit), device_id_type=MESH)

    for load in loads:
        load.start()
    for own in owns:
        own.start()
    angles = [pltpu.make_async_copy(couplings_at, couplings, angle_sem.at[0]), pltpu.make_async_copy(fields_at, fields, angle_sem.at[1])]
    for angle in angles:
        angle.start()
    pl.semaphore_wait(barrier, sum(below) + jnp.where(me < parts // 2, parts - 1, me))
    for n in others:
        target = other(n)

        @pl.when(jnp.logical_and(target < me, target >= parts // 2))
        def _():
            pl.semaphore_signal(far_ready.at[me - parts // 2], inc=1, device_id=across(target), device_id_type=MESH)

    def out(c, n):
        target = other(n)
        return pltpu.make_async_remote_copy(
            src_ref=held.at[target, c] if c < late else state.at[count, c, target],
            dst_ref=mid.at[c, me],
            send_sem=out_send,
            recv_sem=out_recv.at[c],
            device_id=across(target),
            device_id_type=MESH,
        )

    def send(c, k):
        axis, bit, _ = plans[c % 2][k]
        return pltpu.make_async_remote_copy(
            src_ref=state.at[k, c],
            dst_ref=landed.at[k, c],
            send_sem=near_send,
            recv_sem=near_recv.at[k, c // 2],
            device_id=partner(axis, bit),
            device_id_type=MESH,
        )

    tail = sub // TAIL_PARTS
    groups = [(c, 1, 0, sub) for c in range(late)] + [(late, 2, t * tail, tail) for t in range(TAIL_PARTS)]
    pairs = late // 2
    arrivals = [c // 2 for c in range(late)] + [pairs + t for t in range(TAIL_PARTS)]

    def give(g, n):
        c, size, first, length = groups[g]
        span = pl.ds(first, length)
        target = other(n, c < late - 2)
        return pltpu.make_async_remote_copy(
            src_ref=state.at[count, pl.ds(c, size), target, span] if c < late else final.at[:, target, span],
            dst_ref=back.at[me, pl.ds(c, size), span],
            send_sem=back_send,
            recv_sem=back_recv.at[arrivals[g]],
            device_id=across(target),
            device_id_type=MESH,
        )

    def first(low):
        for c in range(AHEAD):
            if low and c == 0:
                loads[c].wait()
            elif low and c == 1:
                settle(held.at[:, pl.ds(1, chunks - 1)], in_sem.at[1])
            for n in others:
                target = other(n)

                known = jnp.logical_or(target < me, me < parts // 2)

                @pl.when(known if low else jnp.logical_not(known))
                def _():
                    if not low and c == 0:
                        pl.semaphore_wait(far_ready.at[target - parts // 2], 1)
                    out(c, n).start()

    first(True)
    for down, (axis, bit, _) in zip(below, near):

        @pl.when(down == 1)
        def _():
            pl.semaphore_signal(near_ready, inc=1, device_id=partner(axis, bit), device_id_type=MESH)

    for angle in angles:
        angle.wait()

    for q in range(qubits):
        cosine[pl.ds(q, 1), :] = jnp.full((1, LANES), fields[q], jnp.float32)
    angles = cosine[...]
    cosine[...] = jnp.cos(angles)
    sine[...] = jnp.sin(angles)

    def angle_of(position, bonds):
        total = jnp.zeros(position.shape, jnp.float32)
        for q in bonds:
            parity = (position >> q ^ position >> ((q + 1) % qubits)) & 1
            total = total + couplings[q] * (1.0 - 2.0 * parity.astype(jnp.float32))
        return total

    quarter = math.pi / 2
    row = lax.broadcasted_iota(jnp.int32, (2 * sub, LANES), 0)
    lane = lax.broadcasted_iota(jnp.int32, (2 * sub, LANES), 1)
    top = jnp.where(row >= sub, 1, 0)
    position = (top << (qubits - 1)) + (((row - top * sub) >> 1) << lane_bits) + lane
    turns = bits_set(position, 0, inner) & 3
    low = angle_of(position, list(range(inner - 1)) + [qubits - 1]) + turns.astype(jnp.float32) * quarter
    low_c[...] = jnp.cos(low)
    low_s[...] = jnp.sin(low)
    table = 2 * parts * chunks
    number = lax.broadcasted_iota(jnp.int32, high_c.shape, 0)
    rest = number - table
    before = rest >= 0
    position = (
        (jnp.where(before, me, number >> (1 + chunk_bits)) << far_first)
        + (near_at << local_bits)
        + (jnp.where(before, rest >> 2, me) << (inner + chunk_bits))
        + (jnp.where(before, late + (rest >> 1 & 1), (number >> 1) & (chunks - 1)) << inner)
        + ((number & 1) << (inner - 1))
    )
    turns = bits_set(position, inner, qubits) & 3
    high = angle_of(position, range(inner - 1, qubits - 1)) + turns.astype(jnp.float32) * quarter
    high_c[...] = jnp.cos(high)
    high_s[...] = jnp.sin(high)
    first(False)

    def turned(value, low_at, high_at):
        sign = jnp.where(lax.broadcasted_iota(jnp.int32, (8, LANES), 0) & 1 == 0, 1.0, -1.0)
        c_low = low_c[pl.ds(pl.multiple_of(low_at, 8), 8), :]
        s_low = low_s[pl.ds(pl.multiple_of(low_at, 8), 8), :]
        c_high = high_c[pl.ds(high_at, 1), :]
        s_high = high_s[pl.ds(high_at, 1), :]
        c_all = c_low * c_high - s_low * s_high
        s_all = s_low * c_high + c_low * s_high
        return value * c_all + swapped(value) * (s_all * sign)

    @pl.loop(0, sub // 8)
    def _(step):
        at = pl.multiple_of(step * 8, 8)
        half = step * 16 // sub
        for c in (late, late + 1):
            for p in range(parts):
                high_at = table + p * 4 + (c - late) * 2 + half
                state[0, c, p, pl.ds(at, 8), :] = turned(held[p, c, pl.ds(at, 8), :], me * 2 // parts * sub + at, high_at)

    @pl.when(sum(below) < count)
    def _():
        pl.semaphore_wait(near_ready, count - sum(below))

    for c in (late, late + 1):
        send(c, 0).start()

    def matrix(shape, first_row, skip, mixed):
        there = lax.broadcasted_iota(jnp.int32, shape, 0) + first_row
        here = lax.broadcasted_iota(jnp.int32, shape, 1)
        total = jnp.ones(shape, jnp.float32)
        if skip:
            total = jnp.where((there ^ here) & ((1 << skip) - 1) == 0, total, 0.0)
        repeat = shape[1] // LANES
        for at, q in enumerate(mixed):
            bit = at + skip
            c_q = jnp.concatenate([cosine[pl.ds(q, 1), :]] * repeat, axis=1)
            s_q = jnp.concatenate([sine[pl.ds(q, 1), :]] * repeat, axis=1)
            up, left = there >> bit & 1, here >> bit & 1
            total = total * jnp.where(up ^ left == 1, s_q, jnp.where(up == 1, -c_q, c_q))
        return total

    lanes_w[...] = matrix((LANES, LANES), 0, 0, range(lane_bits))

    @pl.loop(0, chunk // 8)
    def _(step):
        at = pl.multiple_of(step * 8, 8)
        rows_w[pl.ds(at, 8), :] = matrix((8, chunk), at, 1, list(range(lane_bits, inner)) + list(range(far_first, qubits)))

    def turn(c):
        @pl.loop(0, sub // 8)
        def _(step):
            at = pl.multiple_of(step * 8, 8)
            half = step * 16 // sub
            for p in range(parts):
                mid[c, p, pl.ds(at, 8), :] = turned(mid[c, p, pl.ds(at, 8), :], p * 2 // parts * sub + at, (p * chunks + c) * 2 + half)

    def local(c, target):
        for p in range(parts):
            mid[c, p] = jnp.dot(mid[c, p], lanes_w[...], precision=EXACT, preferred_element_type=jnp.float32)

        @pl.loop(0, parts)
        def _(p):
            at = pl.multiple_of(p * sub, sub)
            target[p] = jnp.dot(
                rows_w[pl.ds(at, sub), :], mid[c].reshape(chunk, LANES), precision=EXACT, preferred_element_type=jnp.float32
            )

    def each_part(step, source, target, straight):
        at = pl.multiple_of(step * 16, 16)
        row = lax.broadcasted_iota(jnp.int32, (16, LANES), 0) + at
        lane = lax.broadcasted_iota(jnp.int32, (16, LANES), 1)
        inside = bits_set(((row >> 1) << lane_bits) + lane, 0, inner) + bits_set(near_at, 0, far_first - local_bits)
        for p in range(parts):
            value = source(p, at)
            if straight:
                turns = inside + p.bit_count()
                value = jnp.where(turns & 1 == 1, swapped(value), value)
                value = jnp.where((turns + (row & 1)) & 2 == 2, -value, value)
            target[p, pl.ds(at, 16), :] = value

    def combine(c, k):
        axis, bit, q = plans[c % 2][k]
        own = 1.0 - 2.0 * ((place[axis] >> bit) & 1).astype(jnp.float32)

        @pl.loop(0, sub // 16)
        def _(step):
            c_q = cosine[pl.ds(q, 1), :] * own
            s_q = sine[pl.ds(q, 1), :]
            source = lambda p, at: c_q * state[k, c, p, pl.ds(at, 16), :] + s_q * landed[k, c, p, pl.ds(at, 16), :]
            each_part(step, source, state.at[k + 1, c], k == count - 1 and c < late)

    def straighten(ref):
        @pl.loop(0, sub // 16)
        def _(step):
            each_part(step, lambda p, at: ref[p, pl.ds(at, 16), :], ref, True)

    def return_all(c):
        sends = [(g, n) for n in others for g, group in enumerate(groups) if group[0] + group[1] - 1 == c]
        for g, n in sends:
            give(g, n).start()

    ARRIVE, MEET, LEAVE = range(3)
    events = [(c, ARRIVE, c, 0) for c in range(chunks)]
    for c in range(1, late, 2):
        events += [(c + STEP * min(k, count - 1) + k // count * 0.2, MEET, c, k) for k in range(1, count + 1)]
    events += [(min(k, count - 1) - 1.5 + k // count * 0.1, MEET, chunks - 1, k) for k in range(1, count + 1)]
    events.append((4 * chunks, LEAVE, chunks - 1, 0))
    for _, what, c, k in sorted(events):
        if what == ARRIVE:
            if c == 0:
                settle(mid.at[pl.ds(0, late), 0], own_sem)
            settle(mid.at[c, pl.ds(0, parts - 1)], out_recv.at[c])
            if c + AHEAD < chunks:
                for n in others:
                    out(c + AHEAD, n).start()
            if c < late:
                turn(c)
                local(c, state.at[0, c])
                send(c, 0).start()
            else:
                mid[c, me] = state[count, c, me]
                local(c, final.at[c - late])
                straighten(final.at[c - late])
                back[me, c] = final[c - late, me]
        elif what == MEET:
            settle(landed.at[k - 1, pl.ds(c - 1, 2)], near_recv.at[k - 1, c // 2])
            for each in (c - 1, c):
                combine(each, k - 1)
                if k < count:
                    send(each, k).start()
                elif c < late:
                    back[me, each] = state[count, each, me]
                    return_all(each)
        else:
            return_all(c)

    settle(mid.at[:, pl.ds(0, parts - 1)], out_send)
    settle(state.at[pl.ds(0, count)], near_send)

    def fold(values, bits, where):
        for bit in bits:
            c_q = cosine[pl.ds(inner + bit, 1), :]
            s_q = sine[pl.ds(inner + bit, 1), :]
            for n in where:
                if not n >> bit & 1:
                    one, two = values[n], values[n | 1 << bit]
                    values[n] = c_q * one + s_q * two
                    values[n | 1 << bit] = s_q * one - c_q * two

    part_span = range(chunk_bits, chunk_bits + part_bits)

    def early(first, length):
        where = [p * chunks + c for p in range(parts) for c in range(first, first + length)]
        inside = [bit for bit in range(chunk_bits) if length >> (bit + 1) and first % (2 << bit) == 0]

        @pl.loop(0, sub // 8)
        def _(step):
            at = pl.multiple_of(step * 8, 8)
            values = {n: back[n // chunks, n % chunks, pl.ds(at, 8), :] for n in where}
            fold(values, inside, where)
            fold(values, part_span, where)
            for n in where:
                back[n // chunks, n % chunks, pl.ds(at, 8), :] = values[n]

    def finish(first, size):
        @pl.loop(0, size // 8)
        def _(step):
            at = pl.multiple_of(first + step * 8, 8)
            sign = jnp.where(lax.broadcasted_iota(jnp.int32, (8, LANES), 0) & 1 == 0, 1.0, -1.0)
            values = [back[n // chunks, n % chunks, pl.ds(at, 8), :] for n in range(parts * chunks)]
            last = [n for n in range(parts * chunks) if n % chunks >= late]
            fold(values, part_span, last)
            fold(values, [0], last)
            for bit in range(1, chunk_bits):
                fold(values, [bit], [n for n in range(parts * chunks) if n % chunks >= chunks - (2 << bit)])
            for n, value in enumerate(values):
                turns = n.bit_count() & 3
                if turns & 1:
                    value = swapped(value) * (sign if turns == 1 else -sign)
                elif turns == 2:
                    value = -value
                done[n // chunks, n % chunks, pl.ds(at, 8), :] = value

    start, size = 0, chunks // 2
    for pair in range(pairs):
        settle(back.at[pl.ds(0, parts - 1), pl.ds(2 * pair, 2)], back_recv.at[pair])
        if start + size == 2 * pair + 2:
            early(start, size)
            start, size = start + size, size // 2
    for t in range(TAIL_PARTS):
        settle(back.at[pl.ds(0, parts - 1), pl.ds(late, 2), pl.ds(t * tail, tail)], back_recv.at[pairs + t])
        finish(t * tail, tail)
    settle(back.at[pl.ds(0, parts - 1)], back_send)


def solution(mesh):
    sizes = {axis: mesh.shape[axis] for axis in AXES}
    count = sum(log2(sizes[axis]) for axis in AXES[1:])

    def step(amplitudes, couplings, fields):
        local = amplitudes.shape[1]
        qubits = couplings.shape[0]
        rows = 2 * local // LANES
        parts = sizes[AXES[0]]
        chunks = 1 << CHUNK_BITS
        sub = rows // (parts * chunks)
        chunk = parts * sub
        table = -(-qubits // 8) * 8
        shape = (parts, chunks, sub, LANES)
        turned = (chunks, parts, sub, LANES)
        woven = amplitudes.reshape(2, local // LANES, LANES).transpose(1, 0, 2).reshape(shape)
        vmem = lambda *shape: pltpu.VMEM(shape, jnp.float32)
        dma = lambda *shape: pltpu.SemaphoreType.DMA(shape)
        result = pl.pallas_call(
            functools.partial(kernel, sizes, qubits),
            out_shape=pltpu.VMEM(shape, jnp.float32),
            in_specs=[pl.BlockSpec(memory_space=pltpu.HBM)] * 3,
            out_specs=pl.BlockSpec(memory_space=pltpu.VMEM),
            scratch_shapes=[
                vmem(*shape),
                vmem(*turned),
                vmem(count + 1, *turned),
                vmem(count, *turned),
                vmem(2, *turned[1:]),
                vmem(*shape),
                vmem(2 * sub, LANES),
                vmem(2 * sub, LANES),
                vmem(2 * parts * (chunks + 2), LANES),
                vmem(2 * parts * (chunks + 2), LANES),
                vmem(table, LANES),
                vmem(table, LANES),
                vmem(chunk, chunk),
                vmem(LANES, LANES),
                pltpu.SMEM((qubits,), jnp.float32),
                pltpu.SMEM((qubits,), jnp.float32),
                pltpu.SemaphoreType.REGULAR((parts // 2,)),
                pltpu.SemaphoreType.REGULAR,
                dma(2),
                dma(2),
                pltpu.SemaphoreType.DMA,
                pltpu.SemaphoreType.DMA,
                dma(chunks),
                pltpu.SemaphoreType.DMA,
                dma(count, chunks // 2),
                pltpu.SemaphoreType.DMA,
                dma(chunks // 2 - 1 + TAIL_PARTS),
            ],
            compiler_params=pltpu.CompilerParams(
                collective_id=0, has_side_effects=True, vmem_limit_bytes=VMEM - 4 * rows * LANES
            ),
        )(couplings, fields, woven)
        return result.reshape(local // LANES, 2, LANES).transpose(1, 0, 2).reshape(2, local)

    placed = (P(None, AXES), P(), P())
    return jax.shard_map(step, mesh=mesh, in_specs=placed, out_specs=P(None, AXES), check_vma=False)
```
